32 devices in a mesh: parts: 2 (over y), slab: 4 (over z), valley: 2 (over x), blk: 2 (over core).
Axes of the slice: x: 2, y: 2, z: 4, core: 2. Of those that a mesh axis runs over, the one named last changes fastest.
Arguments:
- potential: bfloat16 [64, 2048], P('slab'), may hold values from -3.5 to 4
- mode_density: bfloat16 [4, 2048, 2048], P(('parts', 'valley'), 'blk'), parts along dimension 0, may hold values from 0 to 1, as said below
- energy: float32 [4], P(('parts', 'valley')), parts along dimension 0, may hold values from -0.5 to 0.5
- hopping: float32 [4], P(('parts', 'valley')), parts along dimension 0, may hold values from 0.6 to 1.4
- mode_energy: float32 [4, 2048], P(('parts', 'valley'), 'blk'), parts along dimension 0, may hold values from -2.5 to 3
- broadening: float32 [4, 2048], P(('parts', 'valley'), 'blk'), parts along dimension 0, may hold values from 0.0078125 to 0.3
- self_left: float32 [4, 2, 2048], P(('parts', 'valley'), None, 'blk'), parts along dimension 0, may hold values from -1 to 1, as said below
- self_right: float32 [4, 2, 2048], P(('parts', 'valley'), None, 'blk'), parts along dimension 0, may hold values from -1 to 1, as said below
- occupation: float32 [4], P(('parts', 'valley')), parts along dimension 0, may hold values from 0.5 to 1.5
Outputs:
- mode_charge: float32 [4, 64, 2048], P(('parts', 'valley'), 'slab', 'blk'), parts along dimension 0
- electron_density: float32 [128, 2048], P(('parts', 'slab'), ('valley', 'blk')), parts along dimension 0
The draws below stay inside these ranges and needn't reach their ends.
There are 2 independent parts, one for each index of `parts`. The reference program is written for one: setup_inputs(seed, part) draws one part's arguments, and reference() takes and returns one part's arrays. A program takes and returns all parts, laid end to end along the dimension named above; an argument that names none is the same for every part. Nothing has to cross between parts.
Inputs may be any that keep to these rules, and one draw needn't show every extreme that they name: `mode_density`: every entry is positive. `self_left`: the imaginary parts (index 1 of the second dimension) are negative. `self_right`: the imaginary parts (index 1 of the second dimension) are negative.
All inputs are finite; a program needn't handle non-finite values.
Results may differ from the reference program's by a relative error of at most 0.0065.
Values sent between devices are 32-bit elements; how exact they have to be, the bound alone decides.
A program may use at most 64 MiB of HBM per device.

```python
import math
import jax
import jax.numpy as jnp
from jax import lax

WIDTH = 2048
CHAIN = 64
ITEMS = 2


def smooth_bump(places, lower, upper, edge):
    return 0.5 * (jnp.tanh((places - lower) / edge) - jnp.tanh((places - upper) / edge))


def draw_potential(key, part):
    first_key = jax.random.fold_in(key, 17)
    places = (jnp.arange(CHAIN, dtype=jnp.float32) + 0.5) / CHAIN
    edge = 2.0 / CHAIN
    parity = 1.0 - 2.0 * (jnp.arange(CHAIN, dtype=jnp.int32) % 2).astype(jnp.float32)
    double_bump = smooth_bump(places, 0.3, 0.38, edge) + smooth_bump(places, 0.62, 0.7, edge)
    barrier = 0.4 * double_bump
    roughness = jax.random.uniform(first_key, (CHAIN, WIDTH), jnp.float32, -0.6, 0.6)
    row_level = barrier + 2.5 * parity
    return (row_level[:, None] + roughness).astype(jnp.bfloat16)


def draw_mode_density(key, part):
    first_key = jax.random.fold_in(key, 29)
    uniform_part = jax.random.uniform(first_key, (ITEMS, WIDTH, WIDTH), jnp.float32, 0.0, 1.0)
    factors = uniform_part ** 24 + 0.0001
    return (factors / jnp.sum(factors, axis=-1, keepdims=True)).astype(jnp.bfloat16)


def contact_energy(key):
    first_key, second_key = jax.random.split(key)
    real_part = jax.random.uniform(first_key, (ITEMS, WIDTH), jnp.float32, -0.8, 0.8)
    imag_part = -jax.random.uniform(second_key, (ITEMS, WIDTH), jnp.float32, 0.1, 0.9)
    return jnp.stack([real_part, imag_part], axis=1)


def draw_self_left(key, part):
    return contact_energy(jax.random.fold_in(key, 3))


def draw_self_right(key, part):
    return contact_energy(jax.random.fold_in(key, 5))


def level_of(own_key, extent, pieces, least, largest):
    loudness = 1.0
    for axis_at, parts in pieces:
        draws = jax.random.uniform(jax.random.fold_in(jax.random.fold_in(own_key, 6), axis_at), (parts,), jnp.float32, least / len(pieces), largest / len(pieces))
        loudness = loudness * jnp.repeat(jnp.exp(draws), extent[axis_at] // parts).reshape((-1,) + (1,) * (len(extent) - 1 - axis_at))
    return loudness


def setup_inputs(seed: int = 0, part: int = 0) -> dict:
    arg_keys = jax.random.split(jax.random.key(seed), 10)
    part_splits = jax.random.split(jax.random.fold_in(arg_keys[9], part), 10)
    return {
        "potential": draw_potential(jax.random.fold_in(arg_keys[9], 71), part),
        "mode_density": draw_mode_density(jax.random.fold_in(jax.random.fold_in(arg_keys[9], part), 71), part),
        "energy": jnp.clip(jax.random.uniform(part_splits[2], (ITEMS,), jnp.float32, -0.5, 0.5) * level_of(part_splits[2], (ITEMS,), ((0, 2),), -0.4, 0.0), -0.5, 0.5),
        "hopping": jnp.clip(0.6 + 0.79999995 * jax.random.uniform(part_splits[3], (ITEMS,), jnp.float32) ** level_of(part_splits[3], (ITEMS,), ((0, 2),), -0.2, 0.2), 0.6, 1.4),
        "mode_energy": jnp.clip(-2.5 + 5.5 * jax.random.uniform(part_splits[4], (ITEMS, WIDTH), jnp.float32) ** level_of(part_splits[4], (ITEMS, WIDTH), ((0, 2), (1, 2)), -0.2, 0.2), -2.5, 3.0),
        "broadening": jnp.clip(jnp.exp(math.log(0.3) - 3.6480575 * jax.random.uniform(part_splits[5], (ITEMS, WIDTH), jnp.float32) ** level_of(part_splits[5], (ITEMS, WIDTH), ((0, 2), (1, 2)), -0.2, 0.2)), 0.0078125, 0.3),
        "self_left": draw_self_left(jax.random.fold_in(jax.random.fold_in(arg_keys[9], part), 71), part),
        "self_right": draw_self_right(jax.random.fold_in(jax.random.fold_in(arg_keys[9], part), 71), part),
        "occupation": jnp.clip(0.5 + 1.0 * jax.random.uniform(part_splits[8], (ITEMS,), jnp.float32) ** level_of(part_splits[8], (ITEMS,), ((0, 2),), -0.2, 0.2), 0.5, 1.5),
    }


def reference(potential, mode_density, energy, hopping, mode_energy, broadening, self_left, self_right, occupation):
    profile = mode_density.astype(jnp.float32)
    projected = jnp.einsum("inx,sx->isn", profile, potential.astype(jnp.float32))
    onsite_re = energy[:, None, None] - mode_energy[:, None, :] - projected
    onsite_im = jnp.broadcast_to(broadening[:, None, :], projected.shape)
    hop_square = (hopping * hopping)[:, None]

    def sweep(carried, slab_onsite):
        carried_re, carried_im = carried
        slab_re, slab_im = slab_onsite
        bottom_re = slab_re - carried_re
        bottom_im = slab_im - carried_im
        magnitude = bottom_re * bottom_re + bottom_im * bottom_im
        next_re = hop_square * bottom_re / magnitude
        next_im = -hop_square * bottom_im / magnitude
        return (next_re, next_im), (carried_re, carried_im)

    slab_major = (jnp.moveaxis(onsite_re, 1, 0), jnp.moveaxis(onsite_im, 1, 0))
    final_left, (left_re, left_im) = lax.scan(sweep, (self_left[:, 0, :], self_left[:, 1, :]), slab_major)
    final_right, (right_re, right_im) = lax.scan(sweep, (self_right[:, 0, :], self_right[:, 1, :]), slab_major, reverse=True)
    bottom_re = onsite_re - jnp.moveaxis(left_re + right_re, 0, 1)
    bottom_im = onsite_im - jnp.moveaxis(left_im + right_im, 0, 1)
    charge = occupation[:, None, None] / math.pi * bottom_im / (bottom_re * bottom_re + bottom_im * bottom_im)
    charge_half = lax.optimization_barrier(charge.astype(jnp.bfloat16)).astype(jnp.float32)
    density = jnp.einsum("isn,inx->sx", charge_half, profile)
    return charge, density
```

```python
import functools
import math

import jax
import jax.numpy as jnp
from jax import lax
from jax.experimental import pallas as pl
from jax.experimental.pallas import tpu as pltpu
from jax.sharding import PartitionSpec as P

MESH = pl.DeviceIdType.MESH
LANES = 128
PIECE = 256


def times(x, y):
    return x[0] * y[0] - x[1] * y[1], x[0] * y[1] + x[1] * y[0]


def inverse(x):
    scale = 1.0 / (x[0] * x[0] + x[1] * x[1])
    return x[0] * scale, -(x[1] * scale)


def through(near, cross, far, hop_square, term):
    turn = times(near, term)
    share = times(times(cross, term), inverse((1.0 - turn[0], -turn[1])))
    return hop_square * (far[0] + share[0]), hop_square * (far[1] + share[1])


def spread(energy, hopping, occupation, scalars):
    shape = scalars.shape[1:]
    scalars[0] = jnp.full(shape, energy[0])
    scalars[1] = jnp.full(shape, hopping[0] * hopping[0])
    scalars[2] = jnp.full(shape, occupation[0] * (1.0 / math.pi))


def kernel(
    sizes,
    potential,
    profile_at,
    scalars,
    mode_energy_at,
    broadening_at,
    self_left_at,
    self_right_at,
    charge_out,
    density_out,
    mode_energy,
    broadening,
    self_left,
    self_right,
    folded,
    small,
    terms,
    heads,
    tails,
    own,
    others,
    parts_own,
    parts_in,
    send_sem,
    recv_sem,
    send2_sem,
    recv2_sem,
    small_sem,
):
    groups, valleys, blks = sizes
    slabs = potential.shape[0]
    profile = profile_at.at[0]
    modes, width = profile.shape
    rows = modes // LANES
    team = valleys * blks
    columns = width // team
    me = lax.axis_index("slab")
    valley = lax.axis_index("valley")
    blk = lax.axis_index("blk")

    small_loads = [
        pltpu.make_async_copy(source, target, small_sem.at[slot])
        for slot, (source, target) in enumerate(
            [
                (mode_energy_at, mode_energy),
                (broadening_at, broadening),
                (self_left_at, self_left),
                (self_right_at, self_right),
            ]
        )
    ]
    for load in small_loads:
        load.start()

    offsets = [(dv, db) for dv in range(1, valleys) for db in range(blks)]
    offsets += [(0, db) for db in range(1, blks)]
    mates = [(lax.rem(valley + dv, valleys), lax.rem(blk + db, blks)) for dv, db in offsets]
    barrier = pltpu.get_barrier_semaphore()
    for d in range(1, groups):
        pl.semaphore_signal(
            barrier, inc=1, device_id={"slab": lax.rem(me + d, groups)}, device_id_type=MESH
        )
    for tv, tb in mates:
        pl.semaphore_signal(
            barrier, inc=1, device_id={"valley": tv, "blk": tb}, device_id_type=MESH
        )

    size = math.gcd(modes, PIECE)
    for first in range(0, modes, size):
        projected = lax.dot_general(
            potential[...],
            profile[pl.ds(first, size), :],
            (((1,), (1,)), ((), ())),
            preferred_element_type=jnp.float32,
        )
        for j in range(size // LANES):
            row = first // LANES + j
            folded[pl.ds(row, slabs, stride=rows), :] = projected[:, j * LANES : (j + 1) * LANES]

    for load in small_loads:
        load.wait()
    hop_square = scalars[1]
    for j in range(rows):
        span = pl.ds(j * LANES, LANES)
        small[0, pl.ds(j, 1), :] = scalars[0, pl.ds(j, 1), :] - mode_energy[:, span]
        small[1, pl.ds(j, 1), :] = broadening[:, span]
        for part in range(2):
            small[2 + part, pl.ds(j, 1), :] = self_left[0, pl.ds(part, 1), span]
            small[4 + part, pl.ds(j, 1), :] = self_right[0, pl.ds(part, 1), span]

    level = small[0]
    onsite_im = small[1]

    def onsite(s):
        return level - folded[pl.ds(s * rows, rows), :], onsite_im

    def start(s):
        far = inverse(onsite(s))
        return far, times(far, far), far

    def grow(segment, s):
        near, cross, far = segment
        site = onsite(s)
        far = inverse((site[0] - hop_square * far[0], site[1] - hop_square * far[1]))
        linked = times(cross, far)
        linked = hop_square * linked[0], hop_square * linked[1]
        return (near[0] + linked[0], near[1] + linked[1]), times(linked, far), far

    def merge(one, two):
        turn = times(one[2], two[0])
        back = inverse((1.0 - hop_square * turn[0], -(hop_square * turn[1])))
        back = hop_square * back[0], hop_square * back[1]
        more_near = times(times(one[1], two[0]), back)
        more_far = times(times(two[1], one[2]), back)
        near = one[0][0] + more_near[0], one[0][1] + more_near[1]
        far = two[2][0] + more_far[0], two[2][1] + more_far[1]
        cross = times(times(one[1], back), times(two[1], back))
        scale = 1.0 / hop_square
        return near, (scale * cross[0], scale * cross[1]), far

    pieces = []
    run = 4 if slabs % 4 == 0 else slabs
    for first in range(0, slabs, run):
        piece = start(first)
        for s in range(first + 1, first + run):
            piece = grow(piece, s)
        pieces.append(piece)
    while len(pieces) > 1:
        pairs = [merge(x, y) for x, y in zip(pieces[0::2], pieces[1::2])]
        pieces = pairs + pieces[2 * len(pairs) :]
    near, cross, far = pieces[0]
    begin, end = (small[2], small[3]), (small[4], small[5])
    after = through(near, cross, far, hop_square, begin)
    before = through(far, cross, near, hop_square, end)
    is_first, is_last = me == 0, me == groups - 1
    for part in range(2):
        own[part] = jnp.where(is_first, after[part], jnp.where(is_last, before[part], near[part]))
        own[2 + part] = cross[part]
        own[4 + part] = far[part]
        others[0, part] = jnp.where(is_first, begin[part], end[part])

    pl.semaphore_wait(barrier, groups - 1 + team - 1)
    inner = jnp.logical_and(me > 0, me < groups - 1)
    planes = (pl.ds(0, 2), pl.ds(2, 4))
    routes = []
    for distance in range(groups - 1, 0, -1):
        routes.append((me + distance, me - distance, distance))
        routes.append((me - distance, me + distance, groups - distance))
    sends = []
    for target, source, slot in routes:
        copies = [
            pltpu.make_async_remote_copy(
                src_ref=own.at[plane],
                dst_ref=others.at[slot, plane],
                send_sem=send_sem.at[slot, which],
                recv_sem=recv_sem.at[slot, which],
                device_id={"slab": lax.rem(target + groups, groups)},
                device_id_type=MESH,
            )
            for which, plane in enumerate(planes)
        ]
        going = jnp.logical_and(target >= 0, target < groups)
        coming = jnp.logical_and(source >= 0, source < groups)
        full = jnp.logical_and(source > 0, source < groups - 1)
        sends.append((copies, going, coming, full))
    for copies, going, coming, full in sends:

        @pl.when(going)
        def _():
            copies[0].start()

        @pl.when(jnp.logical_and(going, inner))
        def _():
            copies[1].start()

    segment = start(0)
    for s in range(slabs - 1):
        for part in range(6):
            heads[s, part] = segment[part // 2][part % 2]
        if s + 1 < slabs - 1:
            segment = grow(segment, s + 1)
    segment = start(slabs - 1)
    for s in range(slabs - 1, 0, -1):
        for part in range(6):
            tails[s - 1, part] = segment[part // 2][part % 2]
        if s > 1:
            segment = grow(segment, s - 1)

    for copies, going, coming, full in sends:

        @pl.when(coming)
        def _():
            copies[0].wait_recv()

        @pl.when(full)
        def _():
            copies[1].wait_recv()

    def corners(ref, index):
        values = [ref[index, part] for part in range(6)]
        return values[0:2], values[2:4], values[4:6]

    def go_right(k, term):
        near, cross, far = corners(others, me - k)
        return through(near, cross, far, hop_square, term)

    def go_left(step, term):
        near, cross, far = corners(others, step)
        return through(far, cross, near, hop_square, term)

    if groups == 1:
        left, right = begin, end
    else:
        edge = lax.rem(me + 1, groups)
        left = lax.fori_loop(1, me, go_right, (others[me, 0], others[me, 1]))
        right = lax.fori_loop(me + 2, groups, go_left, (others[edge, 0], others[edge, 1]))

    factor = scalars[2]
    for s in range(slabs):
        site = onsite(s)
        a, b = left, right
        if s > 0:
            near, cross, far = corners(heads, s - 1)
            a = through(near, cross, far, hop_square, left)
        if s < slabs - 1:
            near, cross, far = corners(tails, s)
            b = through(near, cross, far, hop_square, right)
        low_re = site[0] - a[0] - b[0]
        low_im = site[1] - a[1] - b[1]
        terms[pl.ds(s * rows, rows), :] = factor * low_im / (low_re * low_re + low_im * low_im)

    for j in range(rows):
        charge_out[0, :, pl.ds(j * LANES, LANES)] = terms[pl.ds(j, slabs, stride=rows), :]
    half = charge_out[0].astype(jnp.bfloat16)

    def share(owner):
        span = pl.ds(pl.multiple_of(owner * columns, columns), columns)
        return jnp.dot(half, profile[:, span], preferred_element_type=jnp.float32)

    sends2 = []
    for slot, (tv, tb) in enumerate(mates):
        parts_own[slot] = share(tv * blks + tb)
        send = pltpu.make_async_remote_copy(
            src_ref=parts_own.at[slot],
            dst_ref=parts_in.at[slot],
            send_sem=send2_sem.at[slot],
            recv_sem=recv2_sem.at[slot],
            device_id={"valley": tv, "blk": tb},
            device_id_type=MESH,
        )
        send.start()
        sends2.append(send)
    total = share(valley * blks + blk)
    for slot in reversed(range(len(mates))):
        sends2[slot].wait_recv()
        total = total + parts_in[slot]
    density_out[...] = total
    for send in sends2:
        send.wait_send()
    for copies, going, coming, full in sends:

        @pl.when(going)
        def _():
            copies[0].wait_send()

        @pl.when(jnp.logical_and(going, inner))
        def _():
            copies[1].wait_send()


def drain(charge, density, charge_out, density_out, sem):
    first = pltpu.make_async_copy(charge, charge_out, sem.at[0])
    second = pltpu.make_async_copy(density, density_out, sem.at[1])
    first.start()
    second.start()
    first.wait()
    second.wait()


def solution(mesh):
    sizes = (mesh.shape["slab"], mesh.shape["valley"], mesh.shape["blk"])
    groups, valleys, blks = sizes
    team = valleys * blks

    def body(
        potential,
        mode_density,
        energy,
        hopping,
        mode_energy,
        broadening,
        self_left,
        self_right,
        occupation,
    ):
        slabs = potential.shape[0]
        modes, width = mode_density.shape[1:]
        rows = modes // LANES
        columns = width // team
        vmem = pl.BlockSpec(memory_space=pltpu.VMEM)
        smem = pl.BlockSpec(memory_space=pltpu.SMEM)
        hbm = pl.BlockSpec(memory_space=pltpu.HBM)
        scalars = pl.pallas_call(
            spread,
            out_shape=pltpu.VMEM((3, rows, LANES), jnp.float32),
            in_specs=[smem] * 3,
            out_specs=vmem,
            cost_estimate=pl.CostEstimate(
                flops=1_600_000_000, bytes_accessed=1 << 16, transcendentals=0
            ),
            compiler_params=pltpu.CompilerParams(vmem_limit_bytes=1024 * 1024),
        )(energy, hopping, occupation)
        smalls = [
            pltpu.with_memory_space_constraint(x, pltpu.HBM)
            for x in (mode_energy, broadening, self_left, self_right)
        ]
        outs = pl.pallas_call(
            functools.partial(kernel, sizes),
            out_shape=(
                pltpu.VMEM((1, slabs, modes), jnp.float32),
                pltpu.VMEM((slabs, columns), jnp.float32),
            ),
            in_specs=[vmem, vmem, vmem, hbm, hbm, hbm, hbm],
            out_specs=(vmem, vmem),
            scratch_shapes=[
                pltpu.VMEM((1, modes), jnp.float32),
                pltpu.VMEM((1, modes), jnp.float32),
                pltpu.VMEM((1, 2, modes), jnp.float32),
                pltpu.VMEM((1, 2, modes), jnp.float32),
                pltpu.VMEM((slabs * rows, LANES), jnp.float32),
                pltpu.VMEM((6, rows, LANES), jnp.float32),
                pltpu.VMEM((slabs * rows, LANES), jnp.float32),
                pltpu.VMEM((max(slabs - 1, 1), 6, rows, LANES), jnp.float32),
                pltpu.VMEM((max(slabs - 1, 1), 6, rows, LANES), jnp.float32),
                pltpu.VMEM((6, rows, LANES), jnp.float32),
                pltpu.VMEM((groups, 6, rows, LANES), jnp.float32),
                pltpu.VMEM((max(team - 1, 1), slabs, columns), jnp.float32),
                pltpu.VMEM((max(team - 1, 1), slabs, columns), jnp.float32),
                pltpu.SemaphoreType.DMA((groups, 2)),
                pltpu.SemaphoreType.DMA((groups, 2)),
                pltpu.SemaphoreType.DMA((max(team - 1, 1),)),
                pltpu.SemaphoreType.DMA((max(team - 1, 1),)),
                pltpu.SemaphoreType.DMA((4,)),
            ],
            compiler_params=pltpu.CompilerParams(
                collective_id=0, has_side_effects=True, vmem_limit_bytes=8 * 1024 * 1024
            ),
        )(potential, mode_density, scalars, *smalls)

        return pl.pallas_call(
            drain,
            out_shape=(
                jax.ShapeDtypeStruct((1, slabs, modes), jnp.float32),
                jax.ShapeDtypeStruct((slabs, columns), jnp.float32),
            ),
            in_specs=[vmem, vmem],
            out_specs=(hbm, hbm),
            scratch_shapes=[pltpu.SemaphoreType.DMA((2,))],
            compiler_params=pltpu.CompilerParams(vmem_limit_bytes=1024 * 1024),
        )(*outs)

    placed = (
        P("slab", None),
        P(("parts", "valley"), "blk", None),
        P(("parts", "valley")),
        P(("parts", "valley")),
        P(("parts", "valley"), "blk"),
        P(("parts", "valley"), "blk"),
        P(("parts", "valley"), None, "blk"),
        P(("parts", "valley"), None, "blk"),
        P(("parts", "valley")),
    )
    return jax.shard_map(
        body,
        mesh=mesh,
        in_specs=placed,
        out_specs=(P(("parts", "valley"), "slab", "blk"), P(("parts", "slab"), ("valley", "blk"))),
        check_vma=False,
    )
```

```python
import functools
import math

import jax
import jax.numpy as jnp
from jax import lax
from jax.experimental import pallas as pl
from jax.experimental.pallas import tpu as pltpu
from jax.sharding import PartitionSpec as P

MESH = pl.DeviceIdType.MESH
LANES = 128
PIECE = 256


def times(x, y):
    return x[0] * y[0] - x[1] * y[1], x[0] * y[1] + x[1] * y[0]


def inverse(x):
    scale = 1.0 / (x[0] * x[0] + x[1] * x[1])
    return x[0] * scale, -(x[1] * scale)


def through(near, cross, far, hop_square, term):
    turn = times(near, term)
    share = times(times(cross, term), inverse((1.0 - turn[0], -turn[1])))
    return hop_square * (far[0] + share[0]), hop_square * (far[1] + share[1])


def portions(valleys, blks, columns):
    return [(slot, 0, columns) for slot in range(valleys * blks - 1)]


def spread(energy, hopping, occupation, scalars):
    shape = scalars.shape[1:]
    scalars[0] = jnp.full(shape, energy[0])
    scalars[1] = jnp.full(shape, hopping[0] * hopping[0])
    scalars[2] = jnp.full(shape, occupation[0] * (1.0 / math.pi))


def kernel(
    sizes,
    potential,
    profile_at,
    scalars,
    mode_energy,
    broadening,
    self_left,
    self_right,
    charge_out,
    density_out,
    folded,
    small,
    terms,
    heads,
    tails,
    own,
    others,
    parts_own,
    parts_in,
    send_sem,
    recv_sem,
    recv2_sem,
):
    groups, valleys, blks = sizes
    slabs = potential.shape[0]
    profile = profile_at.at[0]
    modes, width = profile.shape
    rows = modes // LANES
    team = valleys * blks
    columns = width // team
    me = lax.axis_index("slab")
    valley = lax.axis_index("valley")
    blk = lax.axis_index("blk")

    offsets = [(dv, db) for dv in range(1, valleys) for db in range(blks)]
    offsets += [(0, db) for db in range(1, blks)]
    mates = [(lax.rem(valley + dv, valleys), lax.rem(blk + db, blks)) for dv, db in offsets]
    barrier = pltpu.get_barrier_semaphore()
    for d in range(1, groups):
        pl.semaphore_signal(
            barrier, inc=1, device_id={"slab": lax.rem(me + d, groups)}, device_id_type=MESH
        )
    for tv, tb in mates:
        pl.semaphore_signal(
            barrier, inc=1, device_id={"valley": tv, "blk": tb}, device_id_type=MESH
        )

    size = math.gcd(modes, PIECE)
    for first in range(0, modes, size):
        projected = lax.dot_general(
            potential[...],
            profile[pl.ds(first, size), :],
            (((1,), (1,)), ((), ())),
            preferred_element_type=jnp.float32,
        )
        for j in range(size // LANES):
            row = first // LANES + j
            folded[pl.ds(row, slabs, stride=rows), :] = projected[:, j * LANES : (j + 1) * LANES]

    hop_square = scalars[1]
    for j in range(rows):
        span = pl.ds(j * LANES, LANES)
        small[0, pl.ds(j, 1), :] = scalars[0, pl.ds(j, 1), :] - mode_energy[:, span]
        small[1, pl.ds(j, 1), :] = broadening[:, span]
        for part in range(2):
            small[2 + part, pl.ds(j, 1), :] = self_left[0, pl.ds(part, 1), span]
            small[4 + part, pl.ds(j, 1), :] = self_right[0, pl.ds(part, 1), span]

    level = small[0]
    onsite_im = small[1]

    def onsite(s):
        return level - folded[pl.ds(s * rows, rows), :], onsite_im

    def start(s):
        far = inverse(onsite(s))
        return far, times(far, far), far

    def grow(segment, s):
        near, cross, far = segment
        site = onsite(s)
        far = inverse((site[0] - hop_square * far[0], site[1] - hop_square * far[1]))
        linked = times(cross, far)
        linked = hop_square * linked[0], hop_square * linked[1]
        return (near[0] + linked[0], near[1] + linked[1]), times(linked, far), far

    def merge(one, two):
        turn = times(one[2], two[0])
        back = inverse((1.0 - hop_square * turn[0], -(hop_square * turn[1])))
        back = hop_square * back[0], hop_square * back[1]
        more_near = times(times(one[1], two[0]), back)
        more_far = times(times(two[1], one[2]), back)
        near = one[0][0] + more_near[0], one[0][1] + more_near[1]
        far = two[2][0] + more_far[0], two[2][1] + more_far[1]
        cross = times(times(one[1], back), times(two[1], back))
        scale = 1.0 / hop_square
        return near, (scale * cross[0], scale * cross[1]), far

    pieces = []
    run = 4 if slabs % 4 == 0 else slabs
    for first in range(0, slabs, run):
        piece = start(first)
        for s in range(first + 1, first + run):
            piece = grow(piece, s)
        pieces.append(piece)
    while len(pieces) > 1:
        pairs = [merge(x, y) for x, y in zip(pieces[0::2], pieces[1::2])]
        pieces = pairs + pieces[2 * len(pairs) :]
    near, cross, far = pieces[0]
    begin, end = (small[2], small[3]), (small[4], small[5])
    after = through(near, cross, far, hop_square, begin)
    before = through(far, cross, near, hop_square, end)
    is_first, is_last = me == 0, me == groups - 1
    for part in range(2):
        own[part] = jnp.where(is_first, after[part], jnp.where(is_last, before[part], near[part]))
        own[2 + part] = cross[part]
        own[4 + part] = far[part]
        others[0, part] = jnp.where(is_first, begin[part], end[part])

    pl.semaphore_wait(barrier, groups - 1 + team - 1)
    inner = jnp.logical_and(me > 0, me < groups - 1)
    routes = []
    for distance in range(groups - 1, 0, -1):
        routes.append((me - distance, me + distance, groups - distance))
        routes.append((me + distance, me - distance, distance))
    sends = []
    for target, source, slot in routes:
        short, whole = [
            pltpu.make_async_remote_copy(
                src_ref=own.at[plane],
                dst_ref=others.at[slot, plane],
                send_sem=send_sem.at[slot - 1],
                recv_sem=recv_sem.at[slot - 1],
                device_id={"slab": lax.rem(target + groups, groups)},
                device_id_type=MESH,
            )
            for plane in (pl.ds(0, 2), pl.ds(0, 6))
        ]
        going = jnp.logical_and(target >= 0, target < groups)
        coming = jnp.logical_and(source >= 0, source < groups)
        full = jnp.logical_and(source > 0, source < groups - 1)
        sends.append((short, whole, going, coming, full))
    edge_here = jnp.logical_not(inner)
    for short, whole, going, coming, full in sends:

        @pl.when(jnp.logical_and(going, edge_here))
        def _():
            short.start()

        @pl.when(jnp.logical_and(going, inner))
        def _():
            whole.start()

    segment = start(0)
    for s in range(slabs - 1):
        for part in range(6):
            heads[s, part] = segment[part // 2][part % 2]
        if s + 1 < slabs - 1:
            segment = grow(segment, s + 1)
    segment = start(slabs - 1)
    for s in range(slabs - 1, 0, -1):
        for part in range(6):
            tails[s - 1, part] = segment[part // 2][part % 2]
        if s > 1:
            segment = grow(segment, s - 1)

    for short, whole, going, coming, full in sends:

        @pl.when(jnp.logical_and(going, edge_here))
        def _():
            short.wait_send()

        @pl.when(jnp.logical_and(going, inner))
        def _():
            whole.wait_send()

    for short, whole, going, coming, full in sends:

        @pl.when(jnp.logical_and(coming, jnp.logical_not(full)))
        def _():
            short.wait_recv()

        @pl.when(full)
        def _():
            whole.wait_recv()

    def corners(ref, index):
        values = [ref[index, part] for part in range(6)]
        return values[0:2], values[2:4], values[4:6]

    def go_right(k, term):
        near, cross, far = corners(others, me - k)
        return through(near, cross, far, hop_square, term)

    def go_left(step, term):
        near, cross, far = corners(others, step)
        return through(far, cross, near, hop_square, term)

    if groups == 1:
        left, right = begin, end
    else:
        edge = lax.rem(me + 1, groups)
        left = lax.fori_loop(1, me, go_right, (others[me, 0], others[me, 1]))
        right = lax.fori_loop(me + 2, groups, go_left, (others[edge, 0], others[edge, 1]))

    factor = scalars[2]
    for s in range(slabs):
        site = onsite(s)
        a, b = left, right
        if s > 0:
            near, cross, far = corners(heads, s - 1)
            a = through(near, cross, far, hop_square, left)
        if s < slabs - 1:
            near, cross, far = corners(tails, s)
            b = through(near, cross, far, hop_square, right)
        low_re = site[0] - a[0] - b[0]
        low_im = site[1] - a[1] - b[1]
        terms[pl.ds(s * rows, rows), :] = factor * low_im / (low_re * low_re + low_im * low_im)

    for j in range(rows):
        charge_out[0, :, pl.ds(j * LANES, LANES)] = terms[pl.ds(j, slabs, stride=rows), :]
    half = charge_out[0].astype(jnp.bfloat16)

    def share(owner, first, size):
        span = pl.ds(pl.multiple_of(owner * columns + first, size), size)
        return jnp.dot(half, profile[:, span], preferred_element_type=jnp.float32)

    sends2 = []
    for k, (slot, first, size) in enumerate(portions(valleys, blks, columns)):
        tv, tb = mates[slot]
        span = pl.ds(first, size)
        parts_own[slot, :, span] = share(tv * blks + tb, first, size)
        send = pltpu.make_async_remote_copy(
            src_ref=parts_own.at[slot, :, span],
            dst_ref=parts_in.at[slot, :, span],
            send_sem=send_sem.at[k],
            recv_sem=recv2_sem.at[k],
            device_id={"valley": tv, "blk": tb},
            device_id_type=MESH,
        )
        send.start()
        sends2.append((send, slot, span))
    density_out[...] = share(valley * blks + blk, 0, columns)
    for send, slot, span in reversed(sends2):
        send.wait_recv()
        density_out[:, span] += parts_in[slot, :, span]
    for send, slot, span in sends2:
        send.wait_send()


def drain(charge, density, charge_out, density_out, sem):
    first = pltpu.make_async_copy(charge, charge_out, sem.at[0])
    second = pltpu.make_async_copy(density, density_out, sem.at[1])
    first.start()
    second.start()
    first.wait()
    second.wait()


def solution(mesh):
    sizes = (mesh.shape["slab"], mesh.shape["valley"], mesh.shape["blk"])
    groups, valleys, blks = sizes
    team = valleys * blks

    def body(
        potential,
        mode_density,
        energy,
        hopping,
        mode_energy,
        broadening,
        self_left,
        self_right,
        occupation,
    ):
        slabs = potential.shape[0]
        modes, width = mode_density.shape[1:]
        rows = modes // LANES
        columns = width // team
        pieces = len(portions(valleys, blks, columns))
        vmem = pl.BlockSpec(memory_space=pltpu.VMEM)
        smem = pl.BlockSpec(memory_space=pltpu.SMEM)
        hbm = pl.BlockSpec(memory_space=pltpu.HBM)
        scalars = pl.pallas_call(
            spread,
            out_shape=pltpu.VMEM((3, rows, LANES), jnp.float32),
            in_specs=[smem] * 3,
            out_specs=vmem,
            cost_estimate=pl.CostEstimate(
                flops=1_600_000_000, bytes_accessed=1 << 16, transcendentals=0
            ),
            compiler_params=pltpu.CompilerParams(vmem_limit_bytes=1024 * 1024),
        )(energy, hopping, occupation)
        outs = pl.pallas_call(
            functools.partial(kernel, sizes),
            out_shape=(
                pltpu.VMEM((1, slabs, modes), jnp.float32),
                pltpu.VMEM((slabs, columns), jnp.float32),
            ),
            in_specs=[vmem] * 7,
            out_specs=(vmem, vmem),
            scratch_shapes=[
                pltpu.VMEM((slabs * rows, LANES), jnp.float32),
                pltpu.VMEM((6, rows, LANES), jnp.float32),
                pltpu.VMEM((slabs * rows, LANES), jnp.float32),
                pltpu.VMEM((max(slabs - 1, 1), 6, rows, LANES), jnp.float32),
                pltpu.VMEM((max(slabs - 1, 1), 6, rows, LANES), jnp.float32),
                pltpu.VMEM((6, rows, LANES), jnp.float32),
                pltpu.VMEM((groups, 6, rows, LANES), jnp.float32),
                pltpu.VMEM((max(team - 1, 1), slabs, columns), jnp.float32),
                pltpu.VMEM((max(team - 1, 1), slabs, columns), jnp.float32),
                pltpu.SemaphoreType.DMA((max(groups - 1, pieces, 1),)),
                pltpu.SemaphoreType.DMA((max(groups - 1, 1),)),
                pltpu.SemaphoreType.DMA((max(pieces, 1),)),
            ],
            compiler_params=pltpu.CompilerParams(
                collective_id=0, has_side_effects=True, vmem_limit_bytes=8 * 1024 * 1024
            ),
        )(potential, mode_density, scalars, mode_energy, broadening, self_left, self_right)

        return pl.pallas_call(
            drain,
            out_shape=(
                jax.ShapeDtypeStruct((1, slabs, modes), jnp.float32),
                jax.ShapeDtypeStruct((slabs, columns), jnp.float32),
            ),
            in_specs=[vmem, vmem],
            out_specs=(hbm, hbm),
            scratch_shapes=[pltpu.SemaphoreType.DMA((2,))],
            compiler_params=pltpu.CompilerParams(vmem_limit_bytes=1024 * 1024),
        )(*outs)

    placed = (
        P("slab", None),
        P(("parts", "valley"), "blk", None),
        P(("parts", "valley")),
        P(("parts", "valley")),
        P(("parts", "valley"), "blk"),
        P(("parts", "valley"), "blk"),
        P(("parts", "valley"), None, "blk"),
        P(("parts", "valley"), None, "blk"),
        P(("parts", "valley")),
    )
    return jax.shard_map(
        body,
        mesh=mesh,
        in_specs=placed,
        out_specs=(P(("parts", "valley"), "slab", "blk"), P(("parts", "slab"), ("valley", "blk"))),
        check_vma=False,
    )
```

```python
import functools
import math

import jax
import jax.numpy as jnp
from jax import lax
from jax.experimental import pallas as pl
from jax.experimental.pallas import tpu as pltpu
from jax.sharding import PartitionSpec as P

MESH = pl.DeviceIdType.MESH
LANES = 128
PIECE = 256


def times(x, y):
    return x[0] * y[0] - x[1] * y[1], x[0] * y[1] + x[1] * y[0]


def inverse(x):
    scale = 1.0 / (x[0] * x[0] + x[1] * x[1])
    return x[0] * scale, -(x[1] * scale)


def through(near, cross, far, hop_square, term):
    turn = times(near, term)
    share = times(times(cross, term), inverse((1.0 - turn[0], -turn[1])))
    return hop_square * (far[0] + share[0]), hop_square * (far[1] + share[1])


def portions(valleys, blks, columns):
    return [(slot, 0, columns) for slot in range(valleys * blks - 1)]


def spread(energy, hopping, occupation, scalars):
    shape = scalars.shape[1:]
    scalars[0] = jnp.full(shape, energy[0])
    scalars[1] = jnp.full(shape, hopping[0] * hopping[0])
    scalars[2] = jnp.full(shape, occupation[0] * (1.0 / math.pi))


def kernel(
    sizes,
    potential,
    profile_at,
    scalars,
    mode_energy_at,
    broadening_at,
    self_left_at,
    self_right_at,
    charge_out,
    density_out,
    mode_energy,
    broadening,
    self_left,
    self_right,
    folded,
    small,
    terms,
    heads,
    tails,
    own,
    others,
    parts_own,
    parts_in,
    send_sem,
    recv_sem,
    recv2_sem,
    prepared,
):
    groups, valleys, blks = sizes
    slabs = potential.shape[0]
    profile = profile_at.at[0]
    modes, width = profile.shape
    rows = modes // LANES
    team = valleys * blks
    columns = width // team
    me = lax.axis_index("slab")
    valley = lax.axis_index("valley")
    blk = lax.axis_index("blk")

    small_loads = [
        pltpu.make_async_copy(source, target, send_sem.at[slot])
        for slot, (source, target) in enumerate(
            [
                (mode_energy_at, mode_energy),
                (broadening_at, broadening),
                (self_left_at, self_left),
                (self_right_at, self_right),
            ]
        )
    ]
    for load in small_loads:
        load.start()

    offsets = [(dv, db) for dv in range(1, valleys) for db in range(blks)]
    offsets += [(0, db) for db in range(1, blks)]
    mates = [(lax.rem(valley + dv, valleys), lax.rem(blk + db, blks)) for dv, db in offsets]
    barrier = pltpu.get_barrier_semaphore()
    for d in range(1, groups):
        pl.semaphore_signal(
            barrier, inc=1, device_id={"slab": lax.rem(me + d, groups)}, device_id_type=MESH
        )
    for tv, tb in mates:
        pl.semaphore_signal(
            barrier, inc=1, device_id={"valley": tv, "blk": tb}, device_id_type=MESH
        )

    size = math.gcd(modes, PIECE)
    for first in range(0, modes, size):
        projected = lax.dot_general(
            potential[...],
            profile[pl.ds(first, size), :],
            (((1,), (1,)), ((), ())),
            preferred_element_type=jnp.float32,
        )
        for j in range(size // LANES):
            row = first // LANES + j
            folded[pl.ds(row, slabs, stride=rows), :] = projected[:, j * LANES : (j + 1) * LANES]

    for load in small_loads:
        load.wait()
    hop_square = scalars[1]
    for j in range(rows):
        span = pl.ds(j * LANES, LANES)
        small[0, pl.ds(j, 1), :] = scalars[0, pl.ds(j, 1), :] - mode_energy[:, span]
        small[1, pl.ds(j, 1), :] = broadening[:, span]
        for part in range(2):
            small[2 + part, pl.ds(j, 1), :] = self_left[0, pl.ds(part, 1), span]
            small[4 + part, pl.ds(j, 1), :] = self_right[0, pl.ds(part, 1), span]

    level = small[0]
    onsite_im = small[1]

    def onsite(s):
        return level - folded[pl.ds(s * rows, rows), :], onsite_im

    def start(s):
        far = inverse(onsite(s))
        return far, times(far, far), far

    def grow(segment, s):
        near, cross, far = segment
        site = onsite(s)
        far = inverse((site[0] - hop_square * far[0], site[1] - hop_square * far[1]))
        linked = times(cross, far)
        linked = hop_square * linked[0], hop_square * linked[1]
        return (near[0] + linked[0], near[1] + linked[1]), times(linked, far), far

    def merge(one, two):
        turn = times(one[2], two[0])
        back = inverse((1.0 - hop_square * turn[0], -(hop_square * turn[1])))
        back = hop_square * back[0], hop_square * back[1]
        more_near = times(times(one[1], two[0]), back)
        more_far = times(times(two[1], one[2]), back)
        near = one[0][0] + more_near[0], one[0][1] + more_near[1]
        far = two[2][0] + more_far[0], two[2][1] + more_far[1]
        cross = times(times(one[1], back), times(two[1], back))
        scale = 1.0 / hop_square
        return near, (scale * cross[0], scale * cross[1]), far

    pieces = []
    run = 4 if slabs % 4 == 0 else slabs
    for first in range(0, slabs, run):
        piece = start(first)
        for s in range(first + 1, first + run):
            piece = grow(piece, s)
        pieces.append(piece)
    while len(pieces) > 1:
        pairs = [merge(x, y) for x, y in zip(pieces[0::2], pieces[1::2])]
        pieces = pairs + pieces[2 * len(pairs) :]
    near, cross, far = pieces[0]
    begin, end = (small[2], small[3]), (small[4], small[5])
    after = through(near, cross, far, hop_square, begin)
    before = through(far, cross, near, hop_square, end)
    is_first, is_last = me == 0, me == groups - 1
    for part in range(2):
        own[part] = jnp.where(is_first, after[part], jnp.where(is_last, before[part], near[part]))
        own[2 + part] = cross[part]
        own[4 + part] = far[part]
        others[0, part] = jnp.where(is_first, begin[part], end[part])

    pl.semaphore_wait(barrier, groups - 1 + team - 1)
    inner = jnp.logical_and(me > 0, me < groups - 1)
    routes = []
    for distance in range(groups - 1, 0, -1):
        routes.append((me - distance, me + distance, groups - distance))
        routes.append((me + distance, me - distance, distance))
    sends = []
    for target, source, slot in routes:
        short, whole = [
            pltpu.make_async_remote_copy(
                src_ref=own.at[plane],
                dst_ref=others.at[slot, plane],
                send_sem=send_sem.at[slot - 1],
                recv_sem=recv_sem.at[slot - 1],
                device_id={"slab": lax.rem(target + groups, groups)},
                device_id_type=MESH,
            )
            for plane in (pl.ds(0, 2), pl.ds(0, 6))
        ]
        going = jnp.logical_and(target >= 0, target < groups)
        coming = jnp.logical_and(source >= 0, source < groups)
        full = jnp.logical_and(source > 0, source < groups - 1)
        sends.append((short, whole, going, coming, full))
    edge_here = jnp.logical_not(inner)
    for short, whole, going, coming, full in sends:

        @pl.when(jnp.logical_and(going, edge_here))
        def _():
            short.start()

        @pl.when(jnp.logical_and(going, inner))
        def _():
            whole.start()

    segment = start(0)
    for s in range(slabs - 1):
        for part in range(6):
            heads[s, part] = segment[part // 2][part % 2]
        if s + 1 < slabs - 1:
            segment = grow(segment, s + 1)
    segment = start(slabs - 1)
    for s in range(slabs - 1, 0, -1):
        for part in range(6):
            tails[s - 1, part] = segment[part // 2][part % 2]
        if s > 1:
            segment = grow(segment, s - 1)

    def corners(ref, index):
        values = [ref[index, part] for part in range(6)]
        return values[0:2], values[2:4], values[4:6]

    @pl.when(me == 0)
    def _():
        for s in range(slabs):
            site = onsite(s)
            a = begin
            if s > 0:
                near, cross, far = corners(heads, s - 1)
                a = through(near, cross, far, hop_square, begin)
            ahead = site[0] - a[0], site[1] - a[1]
            slope = ahead
            if s < slabs - 1:
                near, cross, far = corners(tails, s)
                ahead = ahead[0] - hop_square * far[0], ahead[1] - hop_square * far[1]
                slope = times(ahead, near)
                slope = slope[0] + hop_square * cross[0], slope[1] + hop_square * cross[1]
            for part in range(2):
                prepared[s, part] = ahead[part]
                prepared[s, 2 + part] = slope[part]

    for short, whole, going, coming, full in sends:

        @pl.when(jnp.logical_and(going, edge_here))
        def _():
            short.wait_send()

        @pl.when(jnp.logical_and(going, inner))
        def _():
            whole.wait_send()

    for short, whole, going, coming, full in sends:

        @pl.when(jnp.logical_and(coming, jnp.logical_not(full)))
        def _():
            short.wait_recv()

        @pl.when(full)
        def _():
            whole.wait_recv()

    def go_right(k, term):
        near, cross, far = corners(others, me - k)
        return through(near, cross, far, hop_square, term)

    def go_left(step, term):
        near, cross, far = corners(others, step)
        return through(far, cross, near, hop_square, term)

    if groups == 1:
        left, right = begin, end
    else:
        edge = lax.rem(me + 1, groups)
        left = lax.fori_loop(1, me, go_right, (others[me, 0], others[me, 1]))
        right = lax.fori_loop(me + 2, groups, go_left, (others[edge, 0], others[edge, 1]))

    factor = scalars[2]
    @pl.when(me == 0)
    def _():
        for s in range(slabs):
            ahead, slope = [[prepared[s, 2 * k + part] for part in range(2)] for k in range(2)]
            if s < slabs - 1:
                turn = times((tails[s, 0], tails[s, 1]), right)
                drop = times(slope, right)
                up_re, up_im = 1.0 - turn[0], -turn[1]
                low_re, low_im = ahead[0] - drop[0], ahead[1] - drop[1]
                value = up_re * low_im - up_im * low_re
            else:
                low_re, low_im = ahead[0] - right[0], ahead[1] - right[1]
                value = low_im
            terms[pl.ds(s * rows, rows), :] = factor * value / (low_re * low_re + low_im * low_im)

    @pl.when(me != 0)
    def _():
        for s in range(slabs):
            site = onsite(s)
            a, b = left, right
            if s > 0:
                near, cross, far = corners(heads, s - 1)
                a = through(near, cross, far, hop_square, left)
            if s < slabs - 1:
                near, cross, far = corners(tails, s)
                b = through(near, cross, far, hop_square, right)
            low_re = site[0] - a[0] - b[0]
            low_im = site[1] - a[1] - b[1]
            terms[pl.ds(s * rows, rows), :] = factor * low_im / (low_re * low_re + low_im * low_im)

    for j in range(rows):
        charge_out[0, :, pl.ds(j * LANES, LANES)] = terms[pl.ds(j, slabs, stride=rows), :]
    half = charge_out[0].astype(jnp.bfloat16)

    def share(owner, first, size):
        span = pl.ds(pl.multiple_of(owner * columns + first, size), size)
        return jnp.dot(half, profile[:, span], preferred_element_type=jnp.float32)

    sends2 = []
    for k, (slot, first, size) in enumerate(portions(valleys, blks, columns)):
        tv, tb = mates[slot]
        span = pl.ds(first, size)
        parts_own[slot, :, span] = share(tv * blks + tb, first, size)
        send = pltpu.make_async_remote_copy(
            src_ref=parts_own.at[slot, :, span],
            dst_ref=parts_in.at[slot, :, span],
            send_sem=send_sem.at[k],
            recv_sem=recv2_sem.at[k],
            device_id={"valley": tv, "blk": tb},
            device_id_type=MESH,
        )
        send.start()
        sends2.append((send, slot, span))
    density_out[...] = share(valley * blks + blk, 0, columns)
    for send, slot, span in reversed(sends2):
        send.wait_recv()
        density_out[:, span] += parts_in[slot, :, span]
    for send, slot, span in sends2:
        send.wait_send()


def drain(charge, density, charge_out, density_out, sem):
    first = pltpu.make_async_copy(charge, charge_out, sem.at[0])
    second = pltpu.make_async_copy(density, density_out, sem.at[1])
    first.start()
    second.start()
    first.wait()
    second.wait()


def solution(mesh):
    sizes = (mesh.shape["slab"], mesh.shape["valley"], mesh.shape["blk"])
    groups, valleys, blks = sizes
    team = valleys * blks

    def body(
        potential,
        mode_density,
        energy,
        hopping,
        mode_energy,
        broadening,
        self_left,
        self_right,
        occupation,
    ):
        slabs = potential.shape[0]
        modes, width = mode_density.shape[1:]
        rows = modes // LANES
        columns = width // team
        pieces = len(portions(valleys, blks, columns))
        vmem = pl.BlockSpec(memory_space=pltpu.VMEM)
        smem = pl.BlockSpec(memory_space=pltpu.SMEM)
        hbm = pl.BlockSpec(memory_space=pltpu.HBM)
        scalars = pl.pallas_call(
            spread,
            out_shape=pltpu.VMEM((3, rows, LANES), jnp.float32),
            in_specs=[smem] * 3,
            out_specs=vmem,
            cost_estimate=pl.CostEstimate(
                flops=1_600_000_000, bytes_accessed=1 << 16, transcendentals=0
            ),
            compiler_params=pltpu.CompilerParams(vmem_limit_bytes=1024 * 1024),
        )(energy, hopping, occupation)
        smalls = [
            pltpu.with_memory_space_constraint(x, pltpu.HBM)
            for x in (mode_energy, broadening, self_left, self_right)
        ]
        outs = pl.pallas_call(
            functools.partial(kernel, sizes),
            out_shape=(
                pltpu.VMEM((1, slabs, modes), jnp.float32),
                pltpu.VMEM((slabs, columns), jnp.float32),
            ),
            in_specs=[vmem] * 3 + [hbm] * 4,
            out_specs=(vmem, vmem),
            scratch_shapes=[
                pltpu.VMEM((1, modes), jnp.float32),
                pltpu.VMEM((1, modes), jnp.float32),
                pltpu.VMEM((1, 2, modes), jnp.float32),
                pltpu.VMEM((1, 2, modes), jnp.float32),
                pltpu.VMEM((slabs * rows, LANES), jnp.float32),
                pltpu.VMEM((6, rows, LANES), jnp.float32),
                pltpu.VMEM((slabs * rows, LANES), jnp.float32),
                pltpu.VMEM((max(slabs - 1, 1), 6, rows, LANES), jnp.float32),
                pltpu.VMEM((max(slabs - 1, 1), 6, rows, LANES), jnp.float32),
                pltpu.VMEM((6, rows, LANES), jnp.float32),
                pltpu.VMEM((groups, 6, rows, LANES), jnp.float32),
                pltpu.VMEM((max(team - 1, 1), slabs, columns), jnp.float32),
                pltpu.VMEM((max(team - 1, 1), slabs, columns), jnp.float32),
                pltpu.SemaphoreType.DMA((max(groups - 1, pieces, 4),)),
                pltpu.SemaphoreType.DMA((max(groups - 1, 1),)),
                pltpu.SemaphoreType.DMA((max(pieces, 1),)),
                pltpu.VMEM((slabs, 4, rows, LANES), jnp.float32),
            ],
            compiler_params=pltpu.CompilerParams(
                collective_id=0, has_side_effects=True, vmem_limit_bytes=8 * 1024 * 1024
            ),
        )(potential, mode_density, scalars, *smalls)

        return pl.pallas_call(
            drain,
            out_shape=(
                jax.ShapeDtypeStruct((1, slabs, modes), jnp.float32),
                jax.ShapeDtypeStruct((slabs, columns), jnp.float32),
            ),
            in_specs=[vmem, vmem],
            out_specs=(hbm, hbm),
            scratch_shapes=[pltpu.SemaphoreType.DMA((2,))],
            compiler_params=pltpu.CompilerParams(vmem_limit_bytes=1024 * 1024),
        )(*outs)

    placed = (
        P("slab", None),
        P(("parts", "valley"), "blk", None),
        P(("parts", "valley")),
        P(("parts", "valley")),
        P(("parts", "valley"), "blk"),
        P(("parts", "valley"), "blk"),
        P(("parts", "valley"), None, "blk"),
        P(("parts", "valley"), None, "blk"),
        P(("parts", "valley")),
    )
    return jax.shard_map(
        body,
        mesh=mesh,
        in_specs=placed,
        out_specs=(P(("parts", "valley"), "slab", "blk"), P(("parts", "slab"), ("valley", "blk"))),
        check_vma=False,
    )
```

```python
import functools
import math

import jax
import jax.numpy as jnp
from jax import lax
from jax.experimental import pallas as pl
from jax.experimental.pallas import tpu as pltpu
from jax.sharding import PartitionSpec as P

MESH = pl.DeviceIdType.MESH
LANES = 128
PIECE = 512


def times(x, y):
    return x[0] * y[0] - x[1] * y[1], x[0] * y[1] + x[1] * y[0]


def inverse(x):
    scale = 1.0 / (x[0] * x[0] + x[1] * x[1])
    return x[0] * scale, -(x[1] * scale)


def through(near, cross, far, hop_square, term):
    turn = times(near, term)
    share = times(times(cross, term), inverse((1.0 - turn[0], -turn[1])))
    return hop_square * (far[0] + share[0]), hop_square * (far[1] + share[1])


def portions(valleys, blks, columns):
    return [(slot, 0, columns) for slot in range(valleys * blks - 1)]


def spread(energy, hopping, occupation, scalars):
    shape = scalars.shape[1:]
    scalars[0] = jnp.full(shape, energy[0])
    scalars[1] = jnp.full(shape, hopping[0] * hopping[0])
    scalars[2] = jnp.full(shape, occupation[0] * (1.0 / math.pi))


def kernel(
    sizes,
    potential,
    profile_at,
    scalars,
    mode_energy_at,
    broadening_at,
    self_left_at,
    self_right_at,
    charge_out,
    density_out,
    mode_energy,
    broadening,
    self_left,
    self_right,
    folded,
    small,
    terms,
    heads,
    tails,
    own,
    others,
    parts_own,
    parts_in,
    send_sem,
    recv_sem,
    recv2_sem,
    prepared,
    half,
):
    groups, valleys, blks = sizes
    slabs = potential.shape[0]
    profile = profile_at.at[0]
    modes, width = profile.shape
    rows = modes // LANES
    team = valleys * blks
    columns = width // team
    me = lax.axis_index("slab")
    valley = lax.axis_index("valley")
    blk = lax.axis_index("blk")

    small_loads = [
        pltpu.make_async_copy(source, target, send_sem.at[slot])
        for slot, (source, target) in enumerate(
            [
                (mode_energy_at, mode_energy),
                (broadening_at, broadening),
                (self_left_at, self_left),
                (self_right_at, self_right),
            ]
        )
    ]
    for load in small_loads:
        load.start()

    offsets = [(dv, db) for dv in range(1, valleys) for db in range(blks)]
    offsets += [(0, db) for db in range(1, blks)]
    mates = [(lax.rem(valley + dv, valleys), lax.rem(blk + db, blks)) for dv, db in offsets]
    barrier = pltpu.get_barrier_semaphore()
    for d in range(1, groups):
        pl.semaphore_signal(
            barrier, inc=1, device_id={"slab": lax.rem(me + d, groups)}, device_id_type=MESH
        )
    for tv, tb in mates:
        pl.semaphore_signal(
            barrier, inc=1, device_id={"valley": tv, "blk": tb}, device_id_type=MESH
        )

    size = math.gcd(modes, PIECE)
    for first in range(0, modes, size):
        projected = lax.dot_general(
            potential[...],
            profile[pl.ds(first, size), :],
            (((1,), (1,)), ((), ())),
            preferred_element_type=jnp.float32,
        )
        for j in range(size // LANES):
            row = first // LANES + j
            folded[pl.ds(row, slabs, stride=rows), :] = projected[:, j * LANES : (j + 1) * LANES]

    for load in small_loads:
        load.wait()
    hop_square = scalars[1]
    for j in range(rows):
        span = pl.ds(j * LANES, LANES)
        small[0, pl.ds(j, 1), :] = scalars[0, pl.ds(j, 1), :] - mode_energy[:, span]
        small[1, pl.ds(j, 1), :] = broadening[:, span]
        for part in range(2):
            small[2 + part, pl.ds(j, 1), :] = self_left[0, pl.ds(part, 1), span]
            small[4 + part, pl.ds(j, 1), :] = self_right[0, pl.ds(part, 1), span]

    level = small[0]
    onsite_im = small[1]

    def onsite(s):
        return level - folded[pl.ds(s * rows, rows), :], onsite_im

    def start(s):
        far = inverse(onsite(s))
        return far, times(far, far), far

    def grow(segment, s):
        near, cross, far = segment
        site = onsite(s)
        far = inverse((site[0] - hop_square * far[0], site[1] - hop_square * far[1]))
        linked = times(cross, far)
        linked = hop_square * linked[0], hop_square * linked[1]
        return (near[0] + linked[0], near[1] + linked[1]), times(linked, far), far

    def merge(one, two):
        turn = times(one[2], two[0])
        back = inverse((1.0 - hop_square * turn[0], -(hop_square * turn[1])))
        back = hop_square * back[0], hop_square * back[1]
        more_near = times(times(one[1], two[0]), back)
        more_far = times(times(two[1], one[2]), back)
        near = one[0][0] + more_near[0], one[0][1] + more_near[1]
        far = two[2][0] + more_far[0], two[2][1] + more_far[1]
        cross = times(times(one[1], back), times(two[1], back))
        scale = 1.0 / hop_square
        return near, (scale * cross[0], scale * cross[1]), far

    pieces = []
    run = 4 if slabs % 4 == 0 else slabs
    for first in range(0, slabs, run):
        piece = start(first)
        for s in range(first + 1, first + run):
            piece = grow(piece, s)
        pieces.append(piece)
    while len(pieces) > 1:
        pairs = [merge(x, y) for x, y in zip(pieces[0::2], pieces[1::2])]
        pieces = pairs + pieces[2 * len(pairs) :]
    near, cross, far = pieces[0]
    begin, end = (small[2], small[3]), (small[4], small[5])
    after = through(near, cross, far, hop_square, begin)
    before = through(far, cross, near, hop_square, end)
    is_first, is_last = me == 0, me == groups - 1
    for part in range(2):
        own[part] = jnp.where(is_first, after[part], jnp.where(is_last, before[part], near[part]))
        own[2 + part] = cross[part]
        own[4 + part] = far[part]
        others[0, part] = jnp.where(is_first, begin[part], end[part])

    pl.semaphore_wait(barrier, groups - 1 + team - 1)
    inner = jnp.logical_and(me > 0, me < groups - 1)
    routes = []
    for distance in range(groups - 1, 0, -1):
        routes.append((me - distance, me + distance, groups - distance))
        routes.append((me + distance, me - distance, distance))
    sends = []
    for target, source, slot in routes:
        short, whole = [
            pltpu.make_async_remote_copy(
                src_ref=own.at[plane],
                dst_ref=others.at[slot, plane],
                send_sem=send_sem.at[slot - 1],
                recv_sem=recv_sem.at[slot - 1],
                device_id={"slab": lax.rem(target + groups, groups)},
                device_id_type=MESH,
            )
            for plane in (pl.ds(0, 2), pl.ds(0, 6))
        ]
        going = jnp.logical_and(target >= 0, target < groups)
        coming = jnp.logical_and(source >= 0, source < groups)
        full = jnp.logical_and(source > 0, source < groups - 1)
        sends.append((short, whole, going, coming, full))
    edge_here = jnp.logical_not(inner)
    for short, whole, going, coming, full in sends:

        @pl.when(jnp.logical_and(going, edge_here))
        def _():
            short.start()

        @pl.when(jnp.logical_and(going, inner))
        def _():
            whole.start()

    segment = start(0)
    for s in range(slabs - 1):
        for part in range(6):
            heads[s, part] = segment[part // 2][part % 2]
        if s + 1 < slabs - 1:
            segment = grow(segment, s + 1)
    segment = start(slabs - 1)
    for s in range(slabs - 1, 0, -1):
        for part in range(6):
            tails[s - 1, part] = segment[part // 2][part % 2]
        if s > 1:
            segment = grow(segment, s - 1)

    def corners(ref, index):
        values = [ref[index, part] for part in range(6)]
        return values[0:2], values[2:4], values[4:6]

    @pl.when(me == 0)
    def _():
        for s in range(slabs):
            site = onsite(s)
            a = begin
            if s > 0:
                near, cross, far = corners(heads, s - 1)
                a = through(near, cross, far, hop_square, begin)
            ahead = site[0] - a[0], site[1] - a[1]
            slope = ahead
            if s < slabs - 1:
                near, cross, far = corners(tails, s)
                ahead = ahead[0] - hop_square * far[0], ahead[1] - hop_square * far[1]
                slope = times(ahead, near)
                slope = slope[0] + hop_square * cross[0], slope[1] + hop_square * cross[1]
            for part in range(2):
                prepared[s, part] = ahead[part]
                prepared[s, 2 + part] = slope[part]

    for short, whole, going, coming, full in sends:

        @pl.when(jnp.logical_and(going, edge_here))
        def _():
            short.wait_send()

        @pl.when(jnp.logical_and(going, inner))
        def _():
            whole.wait_send()

    for short, whole, going, coming, full in sends:

        @pl.when(jnp.logical_and(coming, jnp.logical_not(full)))
        def _():
            short.wait_recv()

        @pl.when(full)
        def _():
            whole.wait_recv()

    def go_right(k, term):
        near, cross, far = corners(others, me - k)
        return through(near, cross, far, hop_square, term)

    def go_left(step, term):
        near, cross, far = corners(others, step)
        return through(far, cross, near, hop_square, term)

    if groups == 1:
        left, right = begin, end
    else:
        edge = lax.rem(me + 1, groups)
        left = lax.fori_loop(1, me, go_right, (others[me, 0], others[me, 1]))
        right = lax.fori_loop(me + 2, groups, go_left, (others[edge, 0], others[edge, 1]))

    def share(owner, first, size):
        span = pl.ds(pl.multiple_of(owner * columns + first, size), size)
        return jnp.dot(half[...], profile[:, span], preferred_element_type=jnp.float32)

    orders = portions(valleys, blks, columns)

    def contribute():
        for j in range(rows):
            charge_out[0, :, pl.ds(j * LANES, LANES)] = terms[pl.ds(j, slabs, stride=rows), :]
        half[...] = charge_out[0].astype(jnp.bfloat16)
        if orders:
            slot, first, size = orders[0]
            tv, tb = mates[slot]
            parts_own[slot, :, pl.ds(first, size)] = share(tv * blks + tb, first, size)

    factor = scalars[2]
    @pl.when(me == 0)
    def _():
        for s in range(slabs):
            ahead, slope = [[prepared[s, 2 * k + part] for part in range(2)] for k in range(2)]
            if s < slabs - 1:
                turn = times((tails[s, 0], tails[s, 1]), right)
                drop = times(slope, right)
                up_re, up_im = 1.0 - turn[0], -turn[1]
                low_re, low_im = ahead[0] - drop[0], ahead[1] - drop[1]
                value = up_re * low_im - up_im * low_re
            else:
                low_re, low_im = ahead[0] - right[0], ahead[1] - right[1]
                value = low_im
            terms[pl.ds(s * rows, rows), :] = factor * value / (low_re * low_re + low_im * low_im)
        contribute()

    @pl.when(me != 0)
    def _():
        for s in range(slabs):
            site = onsite(s)
            a, b = left, right
            if s > 0:
                near, cross, far = corners(heads, s - 1)
                a = through(near, cross, far, hop_square, left)
            if s < slabs - 1:
                near, cross, far = corners(tails, s)
                b = through(near, cross, far, hop_square, right)
            low_re = site[0] - a[0] - b[0]
            low_im = site[1] - a[1] - b[1]
            terms[pl.ds(s * rows, rows), :] = factor * low_im / (low_re * low_re + low_im * low_im)
        contribute()

    sends2 = []
    for k, (slot, first, size) in enumerate(orders):
        tv, tb = mates[slot]
        span = pl.ds(first, size)
        if k > 0:
            parts_own[slot, :, span] = share(tv * blks + tb, first, size)
        send = pltpu.make_async_remote_copy(
            src_ref=parts_own.at[slot, :, span],
            dst_ref=parts_in.at[slot, :, span],
            send_sem=send_sem.at[k],
            recv_sem=recv2_sem.at[k],
            device_id={"valley": tv, "blk": tb},
            device_id_type=MESH,
        )
        send.start()
        sends2.append((send, slot, span))
    density_out[...] = share(valley * blks + blk, 0, columns)
    for send, slot, span in reversed(sends2):
        send.wait_recv()
        density_out[:, span] += parts_in[slot, :, span]
    for send, slot, span in sends2:
        send.wait_send()


def drain(charge, density, charge_out, density_out, sem):
    first = pltpu.make_async_copy(charge, charge_out, sem.at[0])
    second = pltpu.make_async_copy(density, density_out, sem.at[1])
    first.start()
    second.start()
    first.wait()
    second.wait()


def solution(mesh):
    sizes = (mesh.shape["slab"], mesh.shape["valley"], mesh.shape["blk"])
    groups, valleys, blks = sizes
    team = valleys * blks

    def body(
        potential,
        mode_density,
        energy,
        hopping,
        mode_energy,
        broadening,
        self_left,
        self_right,
        occupation,
    ):
        slabs = potential.shape[0]
        modes, width = mode_density.shape[1:]
        rows = modes // LANES
        columns = width // team
        pieces = len(portions(valleys, blks, columns))
        vmem = pl.BlockSpec(memory_space=pltpu.VMEM)
        smem = pl.BlockSpec(memory_space=pltpu.SMEM)
        hbm = pl.BlockSpec(memory_space=pltpu.HBM)
        scalars = pl.pallas_call(
            spread,
            out_shape=pltpu.VMEM((3, rows, LANES), jnp.float32),
            in_specs=[smem] * 3,
            out_specs=vmem,
            cost_estimate=pl.CostEstimate(
                flops=1_600_000_000, bytes_accessed=1 << 16, transcendentals=0
            ),
            compiler_params=pltpu.CompilerParams(vmem_limit_bytes=1024 * 1024),
        )(energy, hopping, occupation)
        smalls = [
            pltpu.with_memory_space_constraint(x, pltpu.HBM)
            for x in (mode_energy, broadening, self_left, self_right)
        ]
        outs = pl.pallas_call(
            functools.partial(kernel, sizes),
            out_shape=(
                pltpu.VMEM((1, slabs, modes), jnp.float32),
                pltpu.VMEM((slabs, columns), jnp.float32),
            ),
            in_specs=[vmem] * 3 + [hbm] * 4,
            out_specs=(vmem, vmem),
            scratch_shapes=[
                pltpu.VMEM((1, modes), jnp.float32),
                pltpu.VMEM((1, modes), jnp.float32),
                pltpu.VMEM((1, 2, modes), jnp.float32),
                pltpu.VMEM((1, 2, modes), jnp.float32),
                pltpu.VMEM((slabs * rows, LANES), jnp.float32),
                pltpu.VMEM((6, rows, LANES), jnp.float32),
                pltpu.VMEM((slabs * rows, LANES), jnp.float32),
                pltpu.VMEM((max(slabs - 1, 1), 6, rows, LANES), jnp.float32),
                pltpu.VMEM((max(slabs - 1, 1), 6, rows, LANES), jnp.float32),
                pltpu.VMEM((6, rows, LANES), jnp.float32),
                pltpu.VMEM((groups, 6, rows, LANES), jnp.float32),
                pltpu.VMEM((max(team - 1, 1), slabs, columns), jnp.float32),
                pltpu.VMEM((max(team - 1, 1), slabs, columns), jnp.float32),
                pltpu.SemaphoreType.DMA((max(groups - 1, pieces, 4),)),
                pltpu.SemaphoreType.DMA((max(groups - 1, 1),)),
                pltpu.SemaphoreType.DMA((max(pieces, 1),)),
                pltpu.VMEM((slabs, 4, rows, LANES), jnp.float32),
                pltpu.VMEM((slabs, modes), jnp.bfloat16),
            ],
            compiler_params=pltpu.CompilerParams(
                collective_id=0, has_side_effects=True, vmem_limit_bytes=8 * 1024 * 1024
            ),
        )(potential, mode_density, scalars, *smalls)

        return pl.pallas_call(
            drain,
            out_shape=(
                jax.ShapeDtypeStruct((1, slabs, modes), jnp.float32),
                jax.ShapeDtypeStruct((slabs, columns), jnp.float32),
            ),
            in_specs=[vmem, vmem],
            out_specs=(hbm, hbm),
            scratch_shapes=[pltpu.SemaphoreType.DMA((2,))],
            compiler_params=pltpu.CompilerParams(vmem_limit_bytes=1024 * 1024),
        )(*outs)

    placed = (
        P("slab", None),
        P(("parts", "valley"), "blk", None),
        P(("parts", "valley")),
        P(("parts", "valley")),
        P(("parts", "valley"), "blk"),
        P(("parts", "valley"), "blk"),
        P(("parts", "valley"), None, "blk"),
        P(("parts", "valley"), None, "blk"),
        P(("parts", "valley")),
    )
    return jax.shard_map(
        body,
        mesh=mesh,
        in_specs=placed,
        out_specs=(P(("parts", "valley"), "slab", "blk"), P(("parts", "slab"), ("valley", "blk"))),
        check_vma=False,
    )
```

```python
import functools
import math

import jax
import jax.numpy as jnp
from jax import lax
from jax.experimental import pallas as pl
from jax.experimental.pallas import tpu as pltpu
from jax.sharding import PartitionSpec as P

MESH = pl.DeviceIdType.MESH
LANES = 128
PIECE = 512


def times(x, y):
    return x[0] * y[0] - x[1] * y[1], x[0] * y[1] + x[1] * y[0]


def inverse(x):
    scale = 1.0 / (x[0] * x[0] + x[1] * x[1])
    return x[0] * scale, -(x[1] * scale)


def through(near, cross, far, hop_square, term):
    turn = times(near, term)
    share = times(times(cross, term), inverse((1.0 - turn[0], -turn[1])))
    return hop_square * (far[0] + share[0]), hop_square * (far[1] + share[1])


def portions(valleys, blks, columns):
    return [(slot, 0, columns) for slot in range(valleys * blks - 1)]


def spread(energy, hopping, occupation, scalars):
    shape = scalars.shape[1:]
    scalars[0] = jnp.full(shape, energy[0])
    scalars[1] = jnp.full(shape, hopping[0] * hopping[0])
    scalars[2] = jnp.full(shape, occupation[0] * (1.0 / math.pi))


def kernel(
    sizes,
    potential,
    profile_at,
    scalars,
    mode_energy_at,
    broadening_at,
    self_left_at,
    self_right_at,
    charge_out,
    density_out,
    mode_energy,
    broadening,
    self_left,
    self_right,
    folded,
    small,
    terms,
    heads,
    tails,
    own,
    others,
    parts_own,
    parts_in,
    send_sem,
    recv_sem,
    recv2_sem,
    prepared,
):
    groups, valleys, blks = sizes
    slabs = potential.shape[0]
    profile = profile_at.at[0]
    modes, width = profile.shape
    rows = modes // LANES
    team = valleys * blks
    columns = width // team
    me = lax.axis_index("slab")
    valley = lax.axis_index("valley")
    blk = lax.axis_index("blk")

    small_loads = [
        pltpu.make_async_copy(source, target, send_sem.at[slot])
        for slot, (source, target) in enumerate(
            [
                (mode_energy_at, mode_energy),
                (broadening_at, broadening),
                (self_left_at, self_left),
                (self_right_at, self_right),
            ]
        )
    ]
    for load in small_loads:
        load.start()

    offsets = [(dv, db) for dv in range(1, valleys) for db in range(blks)]
    offsets += [(0, db) for db in range(1, blks)]
    mates = [(lax.rem(valley + dv, valleys), lax.rem(blk + db, blks)) for dv, db in offsets]
    barrier = pltpu.get_barrier_semaphore()
    for d in range(1, groups):
        pl.semaphore_signal(
            barrier, inc=1, device_id={"slab": lax.rem(me + d, groups)}, device_id_type=MESH
        )
    for tv, tb in mates:
        pl.semaphore_signal(
            barrier, inc=1, device_id={"valley": tv, "blk": tb}, device_id_type=MESH
        )

    size = math.gcd(modes, PIECE)
    for first in range(0, modes, size):
        projected = lax.dot_general(
            potential[...],
            profile[pl.ds(first, size), :],
            (((1,), (1,)), ((), ())),
            preferred_element_type=jnp.float32,
        )
        for j in range(size // LANES):
            row = first // LANES + j
            folded[pl.ds(row, slabs, stride=rows), :] = projected[:, j * LANES : (j + 1) * LANES]

    for load in small_loads:
        load.wait()
    hop_square = scalars[1]
    for j in range(rows):
        span = pl.ds(j * LANES, LANES)
        small[0, pl.ds(j, 1), :] = scalars[0, pl.ds(j, 1), :] - mode_energy[:, span]
        small[1, pl.ds(j, 1), :] = broadening[:, span]
        for part in range(2):
            small[2 + part, pl.ds(j, 1), :] = self_left[0, pl.ds(part, 1), span]
            small[4 + part, pl.ds(j, 1), :] = self_right[0, pl.ds(part, 1), span]

    level = small[0]
    onsite_im = small[1]

    def onsite(s):
        return level - folded[pl.ds(s * rows, rows), :], onsite_im

    def start(s):
        far = inverse(onsite(s))
        return far, times(far, far), far

    def grow(segment, s):
        near, cross, far = segment
        site = onsite(s)
        far = inverse((site[0] - hop_square * far[0], site[1] - hop_square * far[1]))
        linked = times(cross, far)
        linked = hop_square * linked[0], hop_square * linked[1]
        return (near[0] + linked[0], near[1] + linked[1]), times(linked, far), far

    def merge(one, two):
        turn = times(one[2], two[0])
        back = inverse((1.0 - hop_square * turn[0], -(hop_square * turn[1])))
        back = hop_square * back[0], hop_square * back[1]
        more_near = times(times(one[1], two[0]), back)
        more_far = times(times(two[1], one[2]), back)
        near = one[0][0] + more_near[0], one[0][1] + more_near[1]
        far = two[2][0] + more_far[0], two[2][1] + more_far[1]
        cross = times(times(one[1], back), times(two[1], back))
        scale = 1.0 / hop_square
        return near, (scale * cross[0], scale * cross[1]), far

    pieces = []
    run = 4 if slabs % 4 == 0 else slabs
    for first in range(0, slabs, run):
        piece = start(first)
        for s in range(first + 1, first + run):
            piece = grow(piece, s)
        pieces.append(piece)
    while len(pieces) > 1:
        pairs = [merge(x, y) for x, y in zip(pieces[0::2], pieces[1::2])]
        pieces = pairs + pieces[2 * len(pairs) :]
    near, cross, far = pieces[0]
    begin, end = (small[2], small[3]), (small[4], small[5])
    after = through(near, cross, far, hop_square, begin)
    before = through(far, cross, near, hop_square, end)
    is_first, is_last = me == 0, me == groups - 1
    for part in range(2):
        own[part] = jnp.where(is_first, after[part], jnp.where(is_last, before[part], near[part]))
        own[2 + part] = cross[part]
        own[4 + part] = far[part]
        others[0, part] = jnp.where(is_first, begin[part], end[part])

    pl.semaphore_wait(barrier, groups - 1 + team - 1)
    inner = jnp.logical_and(me > 0, me < groups - 1)
    routes = []
    for distance in range(groups - 1, 0, -1):
        routes.append((me - distance, me + distance, groups - distance))
        routes.append((me + distance, me - distance, distance))
    sends = []
    for target, source, slot in routes:
        short, whole = [
            pltpu.make_async_remote_copy(
                src_ref=own.at[plane],
                dst_ref=others.at[slot, plane],
                send_sem=send_sem.at[slot - 1],
                recv_sem=recv_sem.at[slot - 1],
                device_id={"slab": lax.rem(target + groups, groups)},
                device_id_type=MESH,
            )
            for plane in (pl.ds(0, 2), pl.ds(0, 6))
        ]
        going = jnp.logical_and(target >= 0, target < groups)
        coming = jnp.logical_and(source >= 0, source < groups)
        full = jnp.logical_and(source > 0, source < groups - 1)
        sends.append((short, whole, going, coming, full))
    edge_here = jnp.logical_not(inner)
    for short, whole, going, coming, full in sends:

        @pl.when(jnp.logical_and(going, edge_here))
        def _():
            short.start()

        @pl.when(jnp.logical_and(going, inner))
        def _():
            whole.start()

    segment = start(0)
    for s in range(slabs - 1):
        for part in range(6):
            heads[s, part] = segment[part // 2][part % 2]
        if s + 1 < slabs - 1:
            segment = grow(segment, s + 1)
    segment = start(slabs - 1)
    for s in range(slabs - 1, 0, -1):
        for part in range(6):
            tails[s - 1, part] = segment[part // 2][part % 2]
        if s > 1:
            segment = grow(segment, s - 1)

    def corners(ref, index):
        values = [ref[index, part] for part in range(6)]
        return values[0:2], values[2:4], values[4:6]

    @pl.when(me == 0)
    def _():
        for s in range(slabs):
            site = onsite(s)
            a = begin
            if s > 0:
                near, cross, far = corners(heads, s - 1)
                a = through(near, cross, far, hop_square, begin)
            ahead = site[0] - a[0], site[1] - a[1]
            slope = ahead
            if s < slabs - 1:
                near, cross, far = corners(tails, s)
                ahead = ahead[0] - hop_square * far[0], ahead[1] - hop_square * far[1]
                slope = times(ahead, near)
                slope = slope[0] + hop_square * cross[0], slope[1] + hop_square * cross[1]
            for part in range(2):
                prepared[s, part] = ahead[part]
                prepared[s, 2 + part] = slope[part]

    for short, whole, going, coming, full in sends:

        @pl.when(jnp.logical_and(going, edge_here))
        def _():
            short.wait_send()

        @pl.when(jnp.logical_and(going, inner))
        def _():
            whole.wait_send()

    for short, whole, going, coming, full in sends:

        @pl.when(jnp.logical_and(coming, jnp.logical_not(full)))
        def _():
            short.wait_recv()

        @pl.when(full)
        def _():
            whole.wait_recv()

    def go_right(k, term):
        near, cross, far = corners(others, me - k)
        return through(near, cross, far, hop_square, term)

    def go_left(step, term):
        near, cross, far = corners(others, step)
        return through(far, cross, near, hop_square, term)

    if groups == 1:
        left, right = begin, end
    else:
        edge = lax.rem(me + 1, groups)
        left = lax.fori_loop(1, me, go_right, (others[me, 0], others[me, 1]))
        right = lax.fori_loop(me + 2, groups, go_left, (others[edge, 0], others[edge, 1]))

    factor = scalars[2]
    @pl.when(me == 0)
    def _():
        for s in range(slabs):
            ahead, slope = [[prepared[s, 2 * k + part] for part in range(2)] for k in range(2)]
            if s < slabs - 1:
                turn = times((tails[s, 0], tails[s, 1]), right)
                drop = times(slope, right)
                up_re, up_im = 1.0 - turn[0], -turn[1]
                low_re, low_im = ahead[0] - drop[0], ahead[1] - drop[1]
                value = up_re * low_im - up_im * low_re
            else:
                low_re, low_im = ahead[0] - right[0], ahead[1] - right[1]
                value = low_im
            terms[pl.ds(s * rows, rows), :] = factor * value / (low_re * low_re + low_im * low_im)

    @pl.when(me != 0)
    def _():
        for s in range(slabs):
            site = onsite(s)
            a, b = left, right
            if s > 0:
                near, cross, far = corners(heads, s - 1)
                a = through(near, cross, far, hop_square, left)
            if s < slabs - 1:
                near, cross, far = corners(tails, s)
                b = through(near, cross, far, hop_square, right)
            low_re = site[0] - a[0] - b[0]
            low_im = site[1] - a[1] - b[1]
            terms[pl.ds(s * rows, rows), :] = factor * low_im / (low_re * low_re + low_im * low_im)

    for j in range(rows):
        charge_out[0, :, pl.ds(j * LANES, LANES)] = terms[pl.ds(j, slabs, stride=rows), :]
    half = charge_out[0].astype(jnp.bfloat16)

    def share(owner, first, size):
        span = pl.ds(pl.multiple_of(owner * columns + first, size), size)
        return jnp.dot(half, profile[:, span], preferred_element_type=jnp.float32)

    sends2 = []
    for k, (slot, first, size) in enumerate(portions(valleys, blks, columns)):
        tv, tb = mates[slot]
        span = pl.ds(first, size)
        parts_own[slot, :, span] = share(tv * blks + tb, first, size)
        send = pltpu.make_async_remote_copy(
            src_ref=parts_own.at[slot, :, span],
            dst_ref=parts_in.at[slot, :, span],
            send_sem=send_sem.at[k],
            recv_sem=recv2_sem.at[k],
            device_id={"valley": tv, "blk": tb},
            device_id_type=MESH,
        )
        send.start()
        sends2.append((send, slot, span))
    density_out[...] = share(valley * blks + blk, 0, columns)
    for send, slot, span in reversed(sends2):
        send.wait_recv()
        density_out[:, span] += parts_in[slot, :, span]
    for send, slot, span in sends2:
        send.wait_send()


def drain(charge, density, charge_out, density_out, sem):
    first = pltpu.make_async_copy(charge, charge_out, sem.at[0])
    second = pltpu.make_async_copy(density, density_out, sem.at[1])
    first.start()
    second.start()
    first.wait()
    second.wait()


def solution(mesh):
    sizes = (mesh.shape["slab"], mesh.shape["valley"], mesh.shape["blk"])
    groups, valleys, blks = sizes
    team = valleys * blks

    def body(
        potential,
        mode_density,
        energy,
        hopping,
        mode_energy,
        broadening,
        self_left,
        self_right,
        occupation,
    ):
        slabs = potential.shape[0]
        modes, width = mode_density.shape[1:]
        rows = modes // LANES
        columns = width // team
        pieces = len(portions(valleys, blks, columns))
        vmem = pl.BlockSpec(memory_space=pltpu.VMEM)
        smem = pl.BlockSpec(memory_space=pltpu.SMEM)
        hbm = pl.BlockSpec(memory_space=pltpu.HBM)
        scalars = pl.pallas_call(
            spread,
            out_shape=pltpu.VMEM((3, rows, LANES), jnp.float32),
            in_specs=[smem] * 3,
            out_specs=vmem,
            cost_estimate=pl.CostEstimate(
                flops=1_600_000_000, bytes_accessed=1 << 16, transcendentals=0
            ),
            compiler_params=pltpu.CompilerParams(vmem_limit_bytes=1024 * 1024),
        )(energy, hopping, occupation)
        smalls = [
            pltpu.with_memory_space_constraint(x, pltpu.HBM)
            for x in (mode_energy, broadening, self_left, self_right)
        ]
        outs = pl.pallas_call(
            functools.partial(kernel, sizes),
            out_shape=(
                pltpu.VMEM((1, slabs, modes), jnp.float32),
                pltpu.VMEM((slabs, columns), jnp.float32),
            ),
            in_specs=[vmem] * 3 + [hbm] * 4,
            out_specs=(vmem, vmem),
            scratch_shapes=[
                pltpu.VMEM((1, modes), jnp.float32),
                pltpu.VMEM((1, modes), jnp.float32),
                pltpu.VMEM((1, 2, modes), jnp.float32),
                pltpu.VMEM((1, 2, modes), jnp.float32),
                pltpu.VMEM((slabs * rows, LANES), jnp.float32),
                pltpu.VMEM((6, rows, LANES), jnp.float32),
                pltpu.VMEM((slabs * rows, LANES), jnp.float32),
                pltpu.VMEM((max(slabs - 1, 1), 6, rows, LANES), jnp.float32),
                pltpu.VMEM((max(slabs - 1, 1), 6, rows, LANES), jnp.float32),
                pltpu.VMEM((6, rows, LANES), jnp.float32),
                pltpu.VMEM((groups, 6, rows, LANES), jnp.float32),
                pltpu.VMEM((max(team - 1, 1), slabs, columns), jnp.float32),
                pltpu.VMEM((max(team - 1, 1), slabs, columns), jnp.float32),
                pltpu.SemaphoreType.DMA((max(groups - 1, pieces, 4),)),
                pltpu.SemaphoreType.DMA((max(groups - 1, 1),)),
                pltpu.SemaphoreType.DMA((max(pieces, 1),)),
                pltpu.VMEM((slabs, 4, rows, LANES), jnp.float32),
            ],
            compiler_params=pltpu.CompilerParams(
                collective_id=0, has_side_effects=True, vmem_limit_bytes=8 * 1024 * 1024
            ),
        )(potential, mode_density, scalars, *smalls)

        return pl.pallas_call(
            drain,
            out_shape=(
                jax.ShapeDtypeStruct((1, slabs, modes), jnp.float32),
                jax.ShapeDtypeStruct((slabs, columns), jnp.float32),
            ),
            in_specs=[vmem, vmem],
            out_specs=(hbm, hbm),
            scratch_shapes=[pltpu.SemaphoreType.DMA((2,))],
            compiler_params=pltpu.CompilerParams(vmem_limit_bytes=1024 * 1024),
        )(*outs)

    placed = (
        P("slab", None),
        P(("parts", "valley"), "blk", None),
        P(("parts", "valley")),
        P(("parts", "valley")),
        P(("parts", "valley"), "blk"),
        P(("parts", "valley"), "blk"),
        P(("parts", "valley"), None, "blk"),
        P(("parts", "valley"), None, "blk"),
        P(("parts", "valley")),
    )
    return jax.shard_map(
        body,
        mesh=mesh,
        in_specs=placed,
        out_specs=(P(("parts", "valley"), "slab", "blk"), P(("parts", "slab"), ("valley", "blk"))),
        check_vma=False,
    )
```
